32 devices in a mesh: dp: 2 (over x), sp: 16 (over y, z, core).
Axes of the slice: x: 2, y: 2, z: 4, core: 2. Of those that a mesh axis runs over, the one named last changes fastest.
Arguments:
- x: bfloat16 [4096, 12288], P(('dp', 'sp')), parts along dimension 0
- gain: bfloat16 [12288], replicated
- wq: bfloat16 [12288, 12288], replicated
- wk: bfloat16 [12288, 12288], replicated
- wv: bfloat16 [12288, 12288], replicated
- wo: bfloat16 [12288, 12288], replicated
Outputs:
- output: bfloat16 [4096, 12288], P(('dp', 'sp')), parts along dimension 0
There are 2 independent parts. The reference program is written for one: setup_inputs(seed, part) draws one part's arguments, and reference() takes and returns one part's arrays. A program takes and returns all parts, laid end to end along the dimension named above; an argument that names none is the same for every part.
All inputs are finite; a program needn't handle non-finite values.
Results may differ from the reference program's by a relative error of at most 0.012.
Values are sent between devices in bfloat16 or wider.
A program may use at most 2.75 GiB of HBM per device.

```python
import jax
import jax.numpy as jnp
from jax import lax

ROWS = 2048
D = 12288
HEADS = 96
KV_HEADS = 96
HEAD = 128
THETA = 10000


def setup_inputs(seed: int = 0, part: int = 0) -> dict:
    kx, kn, kq, kk, kv, ko = jax.random.split(jax.random.key(seed), 6)

    def weights(key, rows, columns):
        return jax.random.normal(key, (rows, columns), jnp.float32) * rows**-0.5

    drawn = {
        "x": jax.random.normal(jax.random.fold_in(kx, part), (ROWS, D), jnp.float32),
        "gain": 1 + 0.1 * jax.random.normal(kn, (D,), jnp.float32),
        "wq": 2 * weights(kq, D, HEADS * HEAD),
        "wk": 2 * weights(kk, D, KV_HEADS * HEAD),
        "wv": 4 * weights(kv, D, KV_HEADS * HEAD),
        "wo": weights(ko, HEADS * HEAD, D),
    }
    return {k: v.astype(jnp.bfloat16) for k, v in drawn.items()}


def normed(x, gain):
    wide = x.astype(jnp.float32)
    scale = lax.rsqrt(jnp.mean(wide * wide, -1, keepdims=True) + 1e-6)
    return (wide * scale * gain.astype(jnp.float32)).astype(jnp.bfloat16)


def turned(t, place, theta):
    half = t.shape[-1] // 2
    angle = place.astype(jnp.float32)[:, None] * theta ** (-jnp.arange(half, dtype=jnp.float32) / half)
    cos, sin = jnp.cos(angle)[:, None], jnp.sin(angle)[:, None]
    a, b = t[..., :half].astype(jnp.float32), t[..., half:].astype(jnp.float32)
    return jnp.concatenate([a * cos - b * sin, b * cos + a * sin], -1).astype(jnp.bfloat16)


def matmul(a, w):
    return jnp.dot(a, w, preferred_element_type=jnp.float32).astype(jnp.bfloat16)


def einsum(form, a, b):
    return jnp.einsum(form, a.astype(jnp.float32), b.astype(jnp.float32))


def attention(q, k, v):
    scores = einsum("tgsd,ugd->gstu", q, k) * q.shape[-1] ** -0.5
    token = jnp.arange(q.shape[0])
    scores = jnp.where(token[:, None] >= token, scores, -jnp.inf)
    weights = jax.nn.softmax(scores, -1).astype(jnp.bfloat16)
    return einsum("gstu,ugd->tgsd", weights, v).astype(jnp.bfloat16)


def reference(x, gain, wq, wk, wv, wo):
    a, place = normed(x, gain), jnp.arange(ROWS)
    q = turned(matmul(a, wq).reshape(ROWS, HEADS, HEAD), place, THETA).reshape(ROWS, KV_HEADS, -1, HEAD)
    k = turned(matmul(a, wk).reshape(ROWS, KV_HEADS, HEAD), place, THETA)
    v = matmul(a, wv).reshape(ROWS, KV_HEADS, HEAD)
    seen = attention(q, k, v).reshape(ROWS, HEADS * HEAD)
    return (x.astype(jnp.float32) + jnp.dot(seen, wo, preferred_element_type=jnp.float32)).astype(jnp.bfloat16)
```

```python
import functools

import jax
import jax.numpy as jnp
from jax import lax
from jax.experimental import pallas as pl
from jax.experimental.pallas import tpu as pltpu
from jax.sharding import PartitionSpec as P

HEAD = 128
THETA = 10000
CHIPS = 8
NEG = -1e30
HIDDEN = 2 * NEG
LOG2E = 1.4426950408889634
VMEM = 63 * 2**20
MESH = pl.DeviceIdType.MESH
KCHUNKS = 4
SLOTS = 6
TILES = 12


def _dot(a, b, ca=1, cb=0):
    return lax.dot_general(a, b, (((ca,), (cb,)), ((), ())), preferred_element_type=jnp.float32)


def _partner(chip, far, b0, a):
    z, y = lax.rem(chip, 4), lax.div(chip, 4)
    z1, z0 = lax.div(z, 2), lax.rem(z, 2)
    z1 = z1 + far - 2 * z1 * far
    z0 = z0 + b0 - 2 * z0 * b0
    y = y + a - 2 * y * a
    return 4 * y + 2 * z1 + z0


def _div(i, n):
    return i // n if isinstance(i, int) else lax.div(i, n)


def _rem(i, n):
    return i % n if isinstance(i, int) else lax.rem(i, n)


def _first_order(chip, i):
    k = _div(i, 2)
    return _partner(chip, 1 - _rem(i, 2), _rem(3 - k, 2), _div(3 - k, 2))


def _second_order(chip, i):
    late = _div(i, 6)
    k = _div(i + late, 2) - _div(i, 7)
    return _partner(chip, _rem(i + late, 2), _rem(3 - k, 2), _div(3 - k, 2))


def _meet(core, chip):
    barrier = pltpu.get_barrier_semaphore()
    for i in range(CHIPS - 1):
        pl.semaphore_signal(barrier, inc=1, device_id={"sp": 2 * _first_order(chip, i) + core}, device_id_type=MESH)
    pl.semaphore_signal(barrier, inc=1, device_id={"sp": 2 * chip + 1 - core}, device_id_type=MESH)
    pl.semaphore_wait(barrier, CHIPS)


def _project(x_ref, gain_ref, cos_ref, sin_ref, wq_ref, wk_ref, wv_ref, q_ref, k_ref, v_ref,
             a_s, w_s, acc_s, q_s, k_s, v_s, x_sem, x_send, x_recv, w_sem, send_sem, recv_sem):
    me = lax.axis_index("sp")
    chip, core = lax.div(me, 2), lax.rem(me, 2)
    own, d = x_ref.shape
    nh = q_ref.shape[0]
    wide = nh * HEAD
    deep = d // KCHUNKS
    weights = (wq_ref, wk_ref, wv_ref)

    def fetch(i, t, c):
        first = (core * CHIPS + _first_order(chip, i)) * wide
        return pltpu.make_async_copy(weights[t].at[pl.ds(c * deep, deep), pl.ds(pl.multiple_of(first, HEAD), wide)], w_s.at[c], w_sem.at[c])

    def send(i, t):
        tokens = pl.ds(pl.multiple_of(chip * 2 * own, 2 * own), 2 * own)
        src = (q_s, k_s, v_s)[t].at[i]
        dst = q_ref.at[:, tokens, :] if t == 0 else k_ref.at[:, tokens, :] if t == 1 else v_ref.at[:, :, tokens]
        return src, dst

    def remote(i, t):
        src, dst = send(i, t)
        return pltpu.make_async_remote_copy(src_ref=src, dst_ref=dst, send_sem=send_sem.at[i, t], recv_sem=recv_sem.at[i, t],
                                            device_id={"sp": 2 * _first_order(chip, i) + core}, device_id_type=MESH)

    def local(t):
        src, dst = send(CHIPS - 1, t)
        return pltpu.make_async_copy(src, dst, recv_sem.at[CHIPS - 1, t])

    rows = pl.ds(pl.multiple_of(core * own, own), own)
    mine = pltpu.make_async_copy(x_ref, a_s.at[rows], x_sem)
    mine.start()
    for c in range(KCHUNKS):
        fetch(0, 0, c).start()
    _meet(core, chip)
    swap = pltpu.make_async_remote_copy(src_ref=x_ref, dst_ref=a_s.at[rows], send_sem=x_send, recv_sem=x_recv,
                                        device_id={"sp": 2 * chip + 1 - core}, device_id_type=MESH)
    swap.start()

    def norm(first):
        def some(r, _):
            at = pl.ds(pl.multiple_of(first + r * 16, 16), 16)
            x = a_s[at, :].astype(jnp.float32)
            scale = lax.rsqrt(jnp.mean(x * x, -1, keepdims=True) + 1e-6)
            a_s[at, :] = (a_s[at, :].astype(jnp.float32) * scale * gain_ref[...].astype(jnp.float32)).astype(jnp.bfloat16)
            return 0

        lax.fori_loop(0, own // 16, some, 0)

    mine.wait()
    norm(core * own)
    swap.wait()
    norm((1 - core) * own)

    def start(i, t):
        @pl.when(i < CHIPS - 1)
        def _():
            remote(i, t).start()

        @pl.when(i == CHIPS - 1)
        def _():
            local(t).start()

    def chip_step(i, _):
        for t in range(3):
            acc_s[...] = jnp.zeros_like(acc_s)

            def piece(c, _):
                fetch(i, t, c).wait()
                acc_s[...] += _dot(a_s[:, pl.ds(pl.multiple_of(c * deep, 128), deep)], w_s[c])
                if t < 2:
                    fetch(i, t + 1, c).start()
                else:
                    @pl.when(i < CHIPS - 1)
                    def _():
                        fetch(i + 1, 0, c).start()
                return 0

            lax.fori_loop(0, KCHUNKS, piece, 0)
            if t:
                start(i, t - 1)
            else:
                @pl.when(i > 0)
                def _():
                    remote(i - 1, 2).start()
            for h in range(nh):
                part = acc_s[:, h * HEAD : (h + 1) * HEAD].astype(jnp.bfloat16)
                if t < 2:
                    part = part.astype(jnp.float32)
                    part = (part * cos_ref[...] + pltpu.roll(part, HEAD // 2, 1) * sin_ref[...]).astype(jnp.bfloat16)
                    (q_s, k_s)[t][i, h] = part
                else:
                    v_s[i, h] = part.T
        return 0

    lax.fori_loop(0, CHIPS, chip_step, 0)

    def arrived(i, _):
        for t in range(3):
            remote(i, t).wait()
        return 0

    lax.fori_loop(0, CHIPS - 1, arrived, 0)
    local(2).start()
    for t in range(3):
        local(t).wait()


def _finish(q_ref, k_ref, v_ref, x_ref, wo_ref, y_ref, q_s, k_s, v_s, x_s, o_s, o_r, acc_s, sum_r, w_s, top_s, mix_s, y_s,
            in_sem, w_sem, send_sem, recv_sem, sum_send, sum_recv, out_sem):
    me = lax.axis_index("sp")
    chip, core = lax.div(me, 2), lax.rem(me, 2)
    nh, total, _ = q_ref.shape
    own, d = x_ref.shape
    bq = 2 * own
    wide = nh * HEAD
    cols = d // TILES
    e = HEAD**-0.5 * LOG2E

    order = (0, 2, 4, 7, 1, 3, 5, 6)

    def fetch(n, ct):
        first = (core * CHIPS + _second_order(chip, order[n])) * wide
        slot = _rem(ct, SLOTS)
        return pltpu.make_async_copy(wo_ref.at[pl.ds(pl.multiple_of(first, HEAD), wide), pl.ds(pl.multiple_of(ct * cols, 128), cols)],
                                     w_s.at[slot], w_sem.at[slot])

    ins = [pltpu.make_async_copy(q_ref, q_s, in_sem.at[0]), pltpu.make_async_copy(k_ref, k_s, in_sem.at[1]),
           pltpu.make_async_copy(v_ref, v_s.at[:, :HEAD, :], in_sem.at[2]), pltpu.make_async_copy(x_ref, x_s, in_sem.at[3])]
    for copy in ins:
        copy.start()
    for ct in range(SLOTS):
        fetch(0, ct).start()
    v_s[:, HEAD:, :] = jnp.ones((nh, 16, total), jnp.bfloat16)
    _meet(core, chip)
    for copy in ins[:3]:
        copy.wait()

    def remote(i):
        return pltpu.make_async_remote_copy(src_ref=o_s.at[i], dst_ref=o_r.at[chip], send_sem=send_sem.at[i], recv_sem=recv_sem.at[i],
                                            device_id={"sp": 2 * _second_order(chip, i) + core}, device_id_type=MESH)

    def strip(i, _):
        j = _second_order(chip, i)
        queries = pl.ds(pl.multiple_of(j * bq, bq), bq)

        def block(first, bk, masked):
            keys = pl.ds(pl.multiple_of(first, 256), bk)
            scores = [_dot(k_s[h, keys, :], q_s[h, queries, :], 1, 1) for h in range(nh)]
            if masked:
                ok = lax.broadcasted_iota(jnp.int32, (bk, bq), 0) - (bk - bq) <= lax.broadcasted_iota(jnp.int32, (bk, bq), 1)
            weights, keeps = [], []
            for h, s in enumerate(scores):
                if masked:
                    s = jnp.where(ok, s, HIDDEN)
                old = top_s[h : h + 1, :]
                top = jnp.maximum(old, s.max(axis=0, keepdims=True))
                top_s[h : h + 1, :] = top
                weights.append(jnp.exp2((s - top) * e).astype(jnp.bfloat16))
                keeps.append(jnp.exp2((old - top) * e))
            for h, (p, keep) in enumerate(zip(weights, keeps)):
                mix_s[h] = mix_s[h] * keep + _dot(v_s[h, :, keys], p)

        top_s[...] = jnp.full_like(top_s, NEG)
        mix_s[...] = jnp.zeros_like(mix_s)

        @pl.when(lax.rem(j, 2) == 1)
        def _():
            block((j - 1) * bq, 2 * bq, True)

        @pl.when(lax.rem(j, 2) == 0)
        def _():
            block(j * bq, bq, True)

        @pl.when(i > 0)
        def _():
            remote(i - 1).start()

        lax.fori_loop(0, lax.div(j, 2), lambda n, _: (block(n * 2 * bq, 2 * bq, False), 0)[1], 0)

        def store(ref, at):
            for h in range(nh):
                out = (mix_s[h, :HEAD, :] * (1 / mix_s[h, HEAD : HEAD + 1, :])).T
                ref[at, :, h * HEAD : (h + 1) * HEAD] = out.astype(jnp.bfloat16)

        @pl.when(i < CHIPS - 1)
        def _():
            store(o_s, i)

        @pl.when(i == CHIPS - 1)
        def _():
            store(o_r, chip)

        return 0

    lax.fori_loop(0, CHIPS, strip, 0)

    theirs, mine = (pl.ds(pl.multiple_of(c * own, own), own) for c in (1 - core, core))

    def columns(ct):
        return pl.ds(pl.multiple_of(ct * cols, 128), cols)

    def swap(ct):
        return pltpu.make_async_remote_copy(src_ref=acc_s.at[theirs, columns(ct)], dst_ref=sum_r.at[:, columns(ct)], send_sem=sum_send.at[ct],
                                            recv_sem=sum_recv.at[ct], device_id={"sp": 2 * chip + 1 - core}, device_id_type=MESH)

    for n, i in enumerate(order):
        if i != CHIPS - 1:
            remote(i).wait_recv()
        source = _second_order(chip, i)

        def tile(ct, _):
            fetch(n, ct).wait()
            part = _dot(o_r[source], w_s[lax.rem(ct, SLOTS)])
            if n:
                part += acc_s[:, columns(ct)]
            acc_s[:, columns(ct)] = part

            @pl.when(ct < TILES - SLOTS)
            def _():
                fetch(n, ct + SLOTS).start()

            if n < CHIPS - 1:
                @pl.when(ct >= TILES - SLOTS)
                def _():
                    fetch(n + 1, ct - (TILES - SLOTS)).start()
            else:
                @pl.when(ct > 0)
                def _():
                    swap(ct - 1).start()
            return 0

        lax.fori_loop(0, TILES, tile, 0)

    def result(ct):
        return pltpu.make_async_copy(y_s.at[:, columns(ct)], y_ref.at[:, columns(ct)], out_sem.at[ct])

    def add(ct, _):
        @pl.when(ct == 0)
        def _():
            swap(TILES - 1).start()
            ins[3].wait()

        swap(ct).wait()
        y_s[:, columns(ct)] = (x_s[:, columns(ct)].astype(jnp.float32) + (acc_s[mine, columns(ct)] + sum_r[:, columns(ct)])).astype(jnp.bfloat16)

        @pl.when(ct > 0)
        def _():
            result(ct - 1).start()
        return 0

    lax.fori_loop(0, TILES, add, 0)
    for i in range(CHIPS - 1):
        remote(i).wait_send()
    result(TILES - 1).start()
    for ct in range(TILES):
        result(ct).wait()


def solution(mesh):
    def step(x, gain, wq, wk, wv, wo):
        own, d = x.shape
        nh = wq.shape[1] // (2 * CHIPS * HEAD)
        total = 2 * CHIPS * own
        bf, f32 = jnp.bfloat16, jnp.float32
        hbm = pl.BlockSpec(memory_space=pl.ANY)
        vmem = pl.BlockSpec(memory_space=pltpu.VMEM)
        dma = pltpu.SemaphoreType.DMA

        place = lax.div(lax.axis_index("sp"), 2) * 2 * own + jnp.arange(2 * own)
        half = HEAD // 2
        angle = place.astype(f32)[:, None] * THETA ** (-jnp.arange(half, dtype=f32) / half)
        cos, sin = jnp.cos(angle), jnp.sin(angle)
        cos, sin = jnp.concatenate([cos, cos], 1), jnp.concatenate([-sin, sin], 1)

        heads = jax.ShapeDtypeStruct((nh, total, HEAD), bf)
        q, k, v = pl.pallas_call(
            _project,
            out_shape=[heads, heads, jax.ShapeDtypeStruct((nh, HEAD, total), bf)],
            in_specs=[hbm, vmem, vmem, vmem, hbm, hbm, hbm],
            out_specs=[hbm, hbm, hbm],
            scratch_shapes=[
                pltpu.VMEM((2 * own, d), bf),
                pltpu.VMEM((KCHUNKS, d // KCHUNKS, nh * HEAD), bf),
                pltpu.VMEM((2 * own, nh * HEAD), f32),
                pltpu.VMEM((CHIPS, nh, 2 * own, HEAD), bf),
                pltpu.VMEM((CHIPS, nh, 2 * own, HEAD), bf),
                pltpu.VMEM((CHIPS, nh, HEAD, 2 * own), bf),
                dma, dma, dma, dma((KCHUNKS,)), dma((CHIPS, 3)), dma((CHIPS, 3)),
            ],
            compiler_params=pltpu.CompilerParams(collective_id=0, has_side_effects=True, vmem_limit_bytes=VMEM),
            name="project",
        )(x, gain[None], cos, sin, wq, wk, wv)

        return pl.pallas_call(
            _finish,
            out_shape=jax.ShapeDtypeStruct((own, wo.shape[1]), bf),
            in_specs=[hbm] * 5,
            out_specs=hbm,
            scratch_shapes=[
                pltpu.VMEM((nh, total, HEAD), bf),
                pltpu.VMEM((nh, total, HEAD), bf),
                pltpu.VMEM((nh, HEAD + 16, total), bf),
                pltpu.VMEM((own, d), bf),
                pltpu.VMEM((CHIPS, 2 * own, nh * HEAD), bf),
                pltpu.VMEM((CHIPS, 2 * own, nh * HEAD), bf),
                pltpu.VMEM((2 * own, d), f32),
                pltpu.VMEM((own, d), f32),
                pltpu.VMEM((SLOTS, nh * HEAD, d // TILES), bf),
                pltpu.VMEM((-(-nh // 8) * 8, 2 * own), f32),
                pltpu.VMEM((nh, HEAD + 16, 2 * own), f32),
                pltpu.VMEM((own, d), bf),
                dma((4,)), dma((SLOTS,)), dma((CHIPS,)), dma((CHIPS,)), dma((TILES,)), dma((TILES,)), dma((TILES,)),
            ],
            compiler_params=pltpu.CompilerParams(collective_id=1, has_side_effects=True, vmem_limit_bytes=VMEM),
            name="finish",
        )(q, k, v, x, wo)

    tokens, whole = P(("dp", "sp"), None), P(None, None)
    return jax.shard_map(
        step,
        mesh=mesh,
        in_specs=(tokens, P(None), whole, whole, whole, whole),
        out_specs=tokens,
        check_vma=False,
    )
```

```python
import functools

import jax
import jax.numpy as jnp
from jax import lax
from jax.experimental import pallas as pl
from jax.experimental.pallas import tpu as pltpu
from jax.sharding import PartitionSpec as P

HEAD = 128
THETA = 10000
CHIPS = 8
NEG = -1e30
HIDDEN = 2 * NEG
LOG2E = 1.4426950408889634
VMEM = 63 * 2**20
MESH = pl.DeviceIdType.MESH
KCHUNKS = 4
SLOTS = 6
TILES = 12


def _dot(a, b, ca=1, cb=0):
    return lax.dot_general(a, b, (((ca,), (cb,)), ((), ())), preferred_element_type=jnp.float32)


def _partner(chip, far, b0, a):
    z, y = lax.rem(chip, 4), lax.div(chip, 4)
    z1, z0 = lax.div(z, 2), lax.rem(z, 2)
    z1 = z1 + far - 2 * z1 * far
    z0 = z0 + b0 - 2 * z0 * b0
    y = y + a - 2 * y * a
    return 4 * y + 2 * z1 + z0


def _div(i, n):
    return i // n if isinstance(i, int) else lax.div(i, n)


def _rem(i, n):
    return i % n if isinstance(i, int) else lax.rem(i, n)


def _at_end(chip):
    return 1 - lax.rem(lax.div(lax.rem(chip, 4) + 1, 2), 2)


def _across(chip):
    return _partner(chip, 1, 1, 0)


def _first_order(chip, i):
    end = _at_end(chip)
    far = end * _rem(_div(i + 2, 4), 2)
    b0 = end * (1 - _div(i, 4)) + (1 - end) * (1 - _div(_rem(i, 4), 2))
    return _partner(chip, far, b0, 1 - _rem(i, 2))


def _second_order(chip, i):
    end = _at_end(chip)
    far = end * _rem(_div(i + 2, 4), 2) + (1 - end) * (1 - _div(i, 4))
    b0 = end * (1 - _div(i, 4)) + (1 - end) * (1 - _div(_rem(i, 4), 2))
    return _partner(chip, far, b0, 1 - _rem(i, 2))


def _meet(core, chip):
    barrier = pltpu.get_barrier_semaphore()
    for code in range(1, CHIPS):
        other = _partner(chip, code // 4, code % 2, code // 2 % 2)
        pl.semaphore_signal(barrier, inc=1, device_id={"sp": 2 * other + core}, device_id_type=MESH)
    pl.semaphore_signal(barrier, inc=1, device_id={"sp": 2 * chip + 1 - core}, device_id_type=MESH)
    pl.semaphore_wait(barrier, CHIPS)


def _project(x_ref, gain_ref, cos_ref, sin_ref, wq_ref, wk_ref, wv_ref, q_ref, k_ref, v_ref,
             a_s, w_s, acc_s, q_s, k_s, v_s, x_sem, x_send, x_recv, w_sem, send_sem, recv_sem):
    me = lax.axis_index("sp")
    chip, core = lax.div(me, 2), lax.rem(me, 2)
    middle = _at_end(chip) == 0
    own, d = x_ref.shape
    nh = q_ref.shape[0]
    wide = nh * HEAD
    deep = d // KCHUNKS
    weights = (wq_ref, wk_ref, wv_ref)

    def fetch(i, t, c):
        first = (core * CHIPS + _first_order(chip, i)) * wide
        return pltpu.make_async_copy(weights[t].at[pl.ds(c * deep, deep), pl.ds(pl.multiple_of(first, HEAD), wide)], w_s.at[c], w_sem.at[c])

    def second(i):
        return (1 - _at_end(chip)) * _div(i, 4)

    def place(t, owner):
        tokens = pl.ds(pl.multiple_of(owner * 2 * own, 2 * own), 2 * own)
        return (q_ref, k_ref)[t].at[:, tokens, :] if t < 2 else v_ref.at[:, :, tokens]

    def owner_of(i):
        return chip + second(i) * (_across(chip) - chip)

    def remote(i, t):
        owner = owner_of(i)
        return pltpu.make_async_remote_copy(src_ref=(q_s, k_s, v_s)[t].at[i], dst_ref=place(t, owner), send_sem=send_sem.at[i, t],
                                            recv_sem=recv_sem.at[owner, t], device_id={"sp": 2 * _first_order(chip, i) + core},
                                            device_id_type=MESH)

    def local(i, t):
        owner = owner_of(i)
        return pltpu.make_async_copy((q_s, k_s, v_s)[t].at[i], place(t, owner), recv_sem.at[owner, t])

    def start(i, t):
        here = _first_order(chip, i) == chip

        @pl.when(here)
        def _():
            local(i, t).start()

        @pl.when(jnp.logical_not(here))
        def _():
            remote(i, t).start()

    def block(n):
        return a_s.at[pl.ds(pl.multiple_of(n * own, own), own)]

    def push(n, src, dst, to):
        return pltpu.make_async_remote_copy(src_ref=src, dst_ref=dst, send_sem=x_send.at[n], recv_sem=x_recv.at[n],
                                            device_id={"sp": to}, device_id_type=MESH)

    swap = push(0, x_ref, block(core), 2 * chip + 1 - core)
    cross = push(1, x_ref, block(2 + core), 2 * _across(chip) + core)
    pass_on = push(2, block(2 + core), block(2 + core), 2 * chip + 1 - core)

    mine = pltpu.make_async_copy(x_ref, block(core), x_sem)
    mine.start()
    for c in range(KCHUNKS):
        fetch(0, 0, c).start()
    _meet(core, chip)
    swap.start()

    @pl.when(middle)
    def _():
        cross.start()

    def norm(n):
        def some(r, _):
            at = pl.ds(pl.multiple_of(n * own + r * 16, 16), 16)
            x = a_s[at, :].astype(jnp.float32)
            scale = lax.rsqrt(jnp.mean(x * x, -1, keepdims=True) + 1e-6)
            a_s[at, :] = (a_s[at, :].astype(jnp.float32) * scale * gain_ref[...].astype(jnp.float32)).astype(jnp.bfloat16)
            return 0

        lax.fori_loop(0, own // 16, some, 0)

    mine.wait()
    norm(core)
    swap.wait_recv()
    norm(1 - core)

    def chip_step(i, _):
        @pl.when(middle & (i == 4))
        def _():
            pass_on.wait_send()
            norm(2 + core)
            pass_on.wait_recv()
            norm(3 - core)

        rows = pl.ds(pl.multiple_of(second(i) * 2 * own, 2 * own), 2 * own)
        for t in range(3):
            acc_s[...] = jnp.zeros_like(acc_s)

            def piece(c, _):
                fetch(i, t, c).wait()
                acc_s[...] += _dot(a_s[rows, pl.ds(pl.multiple_of(c * deep, 128), deep)], w_s[c])
                if t < 2:
                    fetch(i, t + 1, c).start()
                else:
                    @pl.when(i < CHIPS - 1)
                    def _():
                        fetch(i + 1, 0, c).start()
                return 0

            lax.fori_loop(0, KCHUNKS, piece, 0)
            if t:
                start(i, t - 1)
            else:
                @pl.when(i > 0)
                def _():
                    start(i - 1, 2)
            for h in range(nh):
                part = acc_s[:, h * HEAD : (h + 1) * HEAD].astype(jnp.bfloat16)
                if t < 2:
                    part = part.astype(jnp.float32)
                    part = (part * cos_ref[rows, :] + pltpu.roll(part, HEAD // 2, 1) * sin_ref[rows, :]).astype(jnp.bfloat16)
                    (q_s, k_s)[t][i, h] = part
                else:
                    v_s[i, h] = part.T
            if t == 1:
                @pl.when(middle & (i == 3))
                def _():
                    cross.wait_recv()
                    pass_on.start()
        return 0

    lax.fori_loop(0, CHIPS, chip_step, 0)
    swap.wait_send()

    @pl.when(middle)
    def _():
        cross.wait_send()

    def sent(i, _):
        @pl.when(_first_order(chip, i) != chip)
        def _():
            for t in range(3):
                remote(i, t).wait_send()
        return 0

    lax.fori_loop(0, CHIPS - 1, sent, 0)
    start(CHIPS - 1, 2)

    def arrived(owner, _):
        for t in range(3):
            pltpu.make_async_copy((q_s, k_s, v_s)[t].at[0], place(t, owner), recv_sem.at[owner, t]).wait()
        return 0

    lax.fori_loop(0, CHIPS, arrived, 0)


def _finish(q_ref, k_ref, v_ref, x_ref, wo_ref, y_ref, q_s, k_s, v_s, x_s, o_s, o_r, acc_s, sum_r, w_s, top_s, mix_s, y_s,
            in_sem, w_sem, send_sem, recv_sem, sum_send, sum_recv, out_sem):
    me = lax.axis_index("sp")
    chip, core = lax.div(me, 2), lax.rem(me, 2)
    nh, total, _ = q_ref.shape
    own, d = x_ref.shape
    bq = 2 * own
    wide = nh * HEAD
    cols = d // TILES
    e = HEAD**-0.5 * LOG2E

    order = ((0, 0, 0), (0, 0, 1), (0, 1, 1), (0, 1, 0), (1, 1, 1), (1, 1, 0), (1, 0, 1), (1, 0, 0))

    def fetch(n, ct):
        first = (core * CHIPS + _partner(chip, *order[n])) * wide
        slot = _rem(ct, SLOTS)
        return pltpu.make_async_copy(wo_ref.at[pl.ds(pl.multiple_of(first, HEAD), wide), pl.ds(pl.multiple_of(ct * cols, 128), cols)],
                                     w_s.at[slot], w_sem.at[slot])

    ins = [pltpu.make_async_copy(q_ref, q_s, in_sem.at[0]), pltpu.make_async_copy(k_ref, k_s, in_sem.at[1]),
           pltpu.make_async_copy(v_ref, v_s.at[:, :HEAD, :], in_sem.at[2]), pltpu.make_async_copy(x_ref, x_s, in_sem.at[3])]
    for copy in ins:
        copy.start()
    for ct in range(SLOTS):
        fetch(0, ct).start()
    v_s[:, HEAD:, :] = jnp.ones((nh, 16, total), jnp.bfloat16)
    _meet(core, chip)
    for copy in ins[:3]:
        copy.wait()

    def remote(i):
        return pltpu.make_async_remote_copy(src_ref=o_s.at[i], dst_ref=o_r.at[chip], send_sem=send_sem.at[i], recv_sem=recv_sem.at[chip],
                                            device_id={"sp": 2 * _second_order(chip, i) + core}, device_id_type=MESH)

    def strip(i, _):
        j = _second_order(chip, i)
        queries = pl.ds(pl.multiple_of(j * bq, bq), bq)

        def block(first, bk, masked):
            keys = pl.ds(pl.multiple_of(first, 256), bk)
            scores = [_dot(k_s[h, keys, :], q_s[h, queries, :], 1, 1) for h in range(nh)]
            if masked:
                ok = lax.broadcasted_iota(jnp.int32, (bk, bq), 0) - (bk - bq) <= lax.broadcasted_iota(jnp.int32, (bk, bq), 1)
            weights, keeps = [], []
            for h, s in enumerate(scores):
                if masked:
                    s = jnp.where(ok, s, HIDDEN)
                old = top_s[h : h + 1, :]
                top = jnp.maximum(old, s.max(axis=0, keepdims=True))
                top_s[h : h + 1, :] = top
                weights.append(jnp.exp2((s - top) * e).astype(jnp.bfloat16))
                keeps.append(jnp.exp2((old - top) * e))
            for h, (p, keep) in enumerate(zip(weights, keeps)):
                mix_s[h] = mix_s[h] * keep + _dot(v_s[h, :, keys], p)

        top_s[...] = jnp.full_like(top_s, NEG)
        mix_s[...] = jnp.zeros_like(mix_s)

        @pl.when(lax.rem(j, 2) == 1)
        def _():
            block((j - 1) * bq, 2 * bq, True)

        @pl.when(lax.rem(j, 2) == 0)
        def _():
            block(j * bq, bq, True)

        @pl.when(i > 0)
        def _():
            remote(i - 1).start()

        lax.fori_loop(0, lax.div(j, 2), lambda n, _: (block(n * 2 * bq, 2 * bq, False), 0)[1], 0)

        def store(ref, at):
            for h in range(nh):
                out = (mix_s[h, :HEAD, :] * (1 / mix_s[h, HEAD : HEAD + 1, :])).T
                ref[at, :, h * HEAD : (h + 1) * HEAD] = out.astype(jnp.bfloat16)

        @pl.when(i < CHIPS - 1)
        def _():
            store(o_s, i)

        @pl.when(i == CHIPS - 1)
        def _():
            store(o_r, chip)

        return 0

    lax.fori_loop(0, CHIPS, strip, 0)

    theirs, mine = (pl.ds(pl.multiple_of(c * own, own), own) for c in (1 - core, core))

    def columns(ct):
        return pl.ds(pl.multiple_of(ct * cols, 128), cols)

    def swap(ct):
        return pltpu.make_async_remote_copy(src_ref=acc_s.at[theirs, columns(ct)], dst_ref=sum_r.at[:, columns(ct)], send_sem=sum_send.at[ct],
                                            recv_sem=sum_recv.at[ct], device_id={"sp": 2 * chip + 1 - core}, device_id_type=MESH)

    for n in range(CHIPS):
        source = _partner(chip, *order[n])
        if n:
            pltpu.make_async_copy(o_s.at[0], o_r.at[source], recv_sem.at[source]).wait()

        def tile(ct, _):
            fetch(n, ct).wait()
            part = _dot(o_r[source], w_s[lax.rem(ct, SLOTS)])
            if n:
                part += acc_s[:, columns(ct)]
            acc_s[:, columns(ct)] = part

            @pl.when(ct < TILES - SLOTS)
            def _():
                fetch(n, ct + SLOTS).start()

            if n < CHIPS - 1:
                @pl.when(ct >= TILES - SLOTS)
                def _():
                    fetch(n + 1, ct - (TILES - SLOTS)).start()
            else:
                @pl.when(ct > 0)
                def _():
                    swap(ct - 1).start()
            return 0

        lax.fori_loop(0, TILES, tile, 0)

    def result(ct):
        return pltpu.make_async_copy(y_s.at[:, columns(ct)], y_ref.at[:, columns(ct)], out_sem.at[ct])

    def add(ct, _):
        @pl.when(ct == 0)
        def _():
            swap(TILES - 1).start()
            ins[3].wait()

        swap(ct).wait()
        y_s[:, columns(ct)] = (x_s[:, columns(ct)].astype(jnp.float32) + (acc_s[mine, columns(ct)] + sum_r[:, columns(ct)])).astype(jnp.bfloat16)

        @pl.when(ct > 0)
        def _():
            result(ct - 1).start()
        return 0

    lax.fori_loop(0, TILES, add, 0)
    for i in range(CHIPS - 1):
        remote(i).wait_send()
    result(TILES - 1).start()
    for ct in range(TILES):
        result(ct).wait()


def solution(mesh):
    def step(x, gain, wq, wk, wv, wo):
        own, d = x.shape
        nh = wq.shape[1] // (2 * CHIPS * HEAD)
        total = 2 * CHIPS * own
        bf, f32 = jnp.bfloat16, jnp.float32
        hbm = pl.BlockSpec(memory_space=pl.ANY)
        vmem = pl.BlockSpec(memory_space=pltpu.VMEM)
        dma = pltpu.SemaphoreType.DMA

        chip = lax.div(lax.axis_index("sp"), 2)
        place = jnp.concatenate([c * 2 * own + jnp.arange(2 * own) for c in (chip, _across(chip))])
        half = HEAD // 2
        angle = place.astype(f32)[:, None] * THETA ** (-jnp.arange(half, dtype=f32) / half)
        cos, sin = jnp.cos(angle), jnp.sin(angle)
        cos, sin = jnp.concatenate([cos, cos], 1), jnp.concatenate([-sin, sin], 1)

        heads = jax.ShapeDtypeStruct((nh, total, HEAD), bf)
        q, k, v = pl.pallas_call(
            _project,
            out_shape=[heads, heads, jax.ShapeDtypeStruct((nh, HEAD, total), bf)],
            in_specs=[hbm, vmem, vmem, vmem, hbm, hbm, hbm],
            out_specs=[hbm, hbm, hbm],
            scratch_shapes=[
                pltpu.VMEM((4 * own, d), bf),
                pltpu.VMEM((KCHUNKS, d // KCHUNKS, nh * HEAD), bf),
                pltpu.VMEM((2 * own, nh * HEAD), f32),
                pltpu.VMEM((CHIPS, nh, 2 * own, HEAD), bf),
                pltpu.VMEM((CHIPS, nh, 2 * own, HEAD), bf),
                pltpu.VMEM((CHIPS, nh, HEAD, 2 * own), bf),
                dma, dma((3,)), dma((3,)), dma((KCHUNKS,)), dma((CHIPS, 3)), dma((CHIPS, 3)),
            ],
            compiler_params=pltpu.CompilerParams(collective_id=0, has_side_effects=True, vmem_limit_bytes=VMEM),
            name="project",
        )(x, gain[None], cos, sin, wq, wk, wv)

        return pl.pallas_call(
            _finish,
            out_shape=jax.ShapeDtypeStruct((own, wo.shape[1]), bf),
            in_specs=[hbm] * 5,
            out_specs=hbm,
            scratch_shapes=[
                pltpu.VMEM((nh, total, HEAD), bf),
                pltpu.VMEM((nh, total, HEAD), bf),
                pltpu.VMEM((nh, HEAD + 16, total), bf),
                pltpu.VMEM((own, d), bf),
                pltpu.VMEM((CHIPS, 2 * own, nh * HEAD), bf),
                pltpu.VMEM((CHIPS, 2 * own, nh * HEAD), bf),
                pltpu.VMEM((2 * own, d), f32),
                pltpu.VMEM((own, d), f32),
                pltpu.VMEM((SLOTS, nh * HEAD, d // TILES), bf),
                pltpu.VMEM((-(-nh // 8) * 8, 2 * own), f32),
                pltpu.VMEM((nh, HEAD + 16, 2 * own), f32),
                pltpu.VMEM((own, d), bf),
                dma((4,)), dma((SLOTS,)), dma((CHIPS,)), dma((CHIPS,)), dma((TILES,)), dma((TILES,)), dma((TILES,)),
            ],
            compiler_params=pltpu.CompilerParams(collective_id=1, has_side_effects=True, vmem_limit_bytes=VMEM),
            name="finish",
        )(q, k, v, x, wo)

    tokens, whole = P(("dp", "sp"), None), P(None, None)
    return jax.shard_map(
        step,
        mesh=mesh,
        in_specs=(tokens, P(None), whole, whole, whole, whole),
        out_specs=tokens,
        check_vma=False,
    )
```

```python
import functools

import jax
import jax.numpy as jnp
from jax import lax
from jax.experimental import pallas as pl
from jax.experimental.pallas import tpu as pltpu
from jax.sharding import PartitionSpec as P

HEAD = 128
THETA = 10000
CHIPS = 8
NEG = -1e30
HIDDEN = 2 * NEG
LOG2E = 1.4426950408889634
VMEM = 63 * 2**20
MESH = pl.DeviceIdType.MESH
KCHUNKS = 4
SLOTS = 6
TILES = 12
LAG = 4


def _dot(a, b, ca=1, cb=0):
    return lax.dot_general(a, b, (((ca,), (cb,)), ((), ())), preferred_element_type=jnp.float32)


def _partner(chip, far, b0, a):
    z, y = lax.rem(chip, 4), lax.div(chip, 4)
    z1, z0 = lax.div(z, 2), lax.rem(z, 2)
    z1 = z1 + far - 2 * z1 * far
    z0 = z0 + b0 - 2 * z0 * b0
    y = y + a - 2 * y * a
    return 4 * y + 2 * z1 + z0


def _div(i, n):
    return i // n if isinstance(i, int) else lax.div(i, n)


def _rem(i, n):
    return i % n if isinstance(i, int) else lax.rem(i, n)


def _at_end(chip):
    return 1 - lax.rem(lax.div(lax.rem(chip, 4) + 1, 2), 2)


def _across(chip):
    return _partner(chip, 1, 1, 0)


def _first_order(chip, i):
    end = _at_end(chip)
    far = end * _rem(_div(i + 2, 4), 2)
    b0 = end * (1 - _div(i, 4)) + (1 - end) * (1 - _div(_rem(i, 4), 2))
    return _partner(chip, far, b0, 1 - _rem(i, 2))


def _second_order(chip, i):
    end, y = _at_end(chip), _div(chip, 4)
    odd, last = _rem(i, 2), _div(i, 6)
    far = end * _rem(_div(i + 2, 4), 2) + (1 - end) * (1 - _div(i, 4))
    b0 = end * (1 - _div(i, 4)) + (1 - end) * (1 - _div(_rem(i, 4), 2))
    return _partner(chip, far, b0, last * (1 - odd) + (1 - last) * (y + odd - 2 * y * odd))


def _meet(core, chip):
    barrier = pltpu.get_barrier_semaphore()
    for code in range(1, CHIPS):
        other = _partner(chip, code // 4, code % 2, code // 2 % 2)
        pl.semaphore_signal(barrier, inc=1, device_id={"sp": 2 * other + core}, device_id_type=MESH)
    pl.semaphore_signal(barrier, inc=1, device_id={"sp": 2 * chip + 1 - core}, device_id_type=MESH)
    pl.semaphore_wait(barrier, CHIPS)


def _project(x_ref, gain_ref, cos_ref, sin_ref, wq_ref, wk_ref, wv_ref, q_ref, k_ref, v_ref,
             a_s, w_s, acc_s, q_s, k_s, v_s, gain_s, cos_s, sin_s, x_sem, x_send, x_recv, w_sem, send_sem, recv_sem):
    me = lax.axis_index("sp")
    chip, core = lax.div(me, 2), lax.rem(me, 2)
    middle = _at_end(chip) == 0
    own, d = x_ref.shape
    nh = q_ref.shape[0]
    wide = nh * HEAD
    deep = d // KCHUNKS
    weights = (wq_ref, wk_ref, wv_ref)

    def fetch(i, t, c):
        first = (core * CHIPS + _first_order(chip, i)) * wide
        return pltpu.make_async_copy(weights[t].at[pl.ds(c * deep, deep), pl.ds(pl.multiple_of(first, HEAD), wide)], w_s.at[c], w_sem.at[c])

    def second(i):
        return (1 - _at_end(chip)) * _div(i, 4)

    def place(t, owner):
        tokens = pl.ds(pl.multiple_of(owner * 2 * own, 2 * own), 2 * own)
        return (q_ref, k_ref)[t].at[:, tokens, :] if t < 2 else v_ref.at[:, :, tokens]

    def owner_of(i):
        return chip + second(i) * (_across(chip) - chip)

    def remote(i, t):
        owner = owner_of(i)
        return pltpu.make_async_remote_copy(src_ref=(q_s, k_s, v_s)[t].at[i], dst_ref=place(t, owner), send_sem=send_sem.at[i, t],
                                            recv_sem=recv_sem.at[owner, t], device_id={"sp": 2 * _first_order(chip, i) + core},
                                            device_id_type=MESH)

    def local(i, t):
        owner = owner_of(i)
        return pltpu.make_async_copy((q_s, k_s, v_s)[t].at[i], place(t, owner), recv_sem.at[owner, t])

    def start(i, t):
        here = _first_order(chip, i) == chip

        @pl.when(here)
        def _():
            local(i, t).start()

        @pl.when(jnp.logical_not(here))
        def _():
            remote(i, t).start()

    def block(n):
        return a_s.at[pl.ds(pl.multiple_of(n * own, own), own)]

    def push(n, src, dst, to):
        return pltpu.make_async_remote_copy(src_ref=src, dst_ref=dst, send_sem=x_send.at[n], recv_sem=x_recv.at[n],
                                            device_id={"sp": to}, device_id_type=MESH)

    swap = push(0, x_ref, block(core), 2 * chip + 1 - core)
    cross = push(1, x_ref, block(2 + core), 2 * _across(chip) + core)
    pass_on = push(2, block(2 + core), block(2 + core), 2 * chip + 1 - core)

    mine = pltpu.make_async_copy(x_ref, block(core), x_sem)
    mine.start()
    for c in range(KCHUNKS):
        fetch(0, 0, c).start()
    _meet(core, chip)
    swap.start()

    @pl.when(middle)
    def _():
        cross.start()

    gain_s[...] = jnp.concatenate([gain_ref[n : n + 1, :] for n in range(d // 128)], 1).astype(jnp.float32)
    cos_s[...] = jnp.concatenate([cos_ref[...], cos_ref[...]], 1)
    sin_s[...] = jnp.concatenate([-sin_ref[...], sin_ref[...]], 1)

    def norm(n):
        def some(r, _):
            at = pl.ds(pl.multiple_of(n * own + r * 16, 16), 16)
            x = a_s[at, :].astype(jnp.float32)
            scale = lax.rsqrt(jnp.mean(x * x, -1, keepdims=True) + 1e-6)
            a_s[at, :] = (a_s[at, :].astype(jnp.float32) * scale * gain_s[...]).astype(jnp.bfloat16)
            return 0

        lax.fori_loop(0, own // 16, some, 0)

    mine.wait()
    norm(core)
    swap.wait_recv()
    norm(1 - core)

    def chip_step(i, _):
        @pl.when(middle & (i == 4))
        def _():
            pass_on.wait_send()
            norm(2 + core)
            pass_on.wait_recv()
            norm(3 - core)

        rows = pl.ds(pl.multiple_of(second(i) * 2 * own, 2 * own), 2 * own)
        for t in range(3):
            acc_s[...] = jnp.zeros_like(acc_s)

            def piece(c, _):
                fetch(i, t, c).wait()
                acc_s[...] += _dot(a_s[rows, pl.ds(pl.multiple_of(c * deep, 128), deep)], w_s[c])
                if t < 2:
                    fetch(i, t + 1, c).start()
                else:
                    @pl.when(i < CHIPS - 1)
                    def _():
                        fetch(i + 1, 0, c).start()
                return 0

            lax.fori_loop(0, KCHUNKS, piece, 0)
            if t:
                start(i, t - 1)
            else:
                @pl.when(i > 0)
                def _():
                    start(i - 1, 2)
            for h in range(nh):
                part = acc_s[:, h * HEAD : (h + 1) * HEAD].astype(jnp.bfloat16)
                if t < 2:
                    part = part.astype(jnp.float32)
                    part = (part * cos_s[rows, :] + pltpu.roll(part, HEAD // 2, 1) * sin_s[rows, :]).astype(jnp.bfloat16)
                    (q_s, k_s)[t][i, h] = part
                else:
                    v_s[i, h] = part.T
            if t == 1:
                @pl.when(middle & (i == 3))
                def _():
                    cross.wait_recv()
                    pass_on.start()
        return 0

    lax.fori_loop(0, CHIPS, chip_step, 0)
    swap.wait_send()

    @pl.when(middle)
    def _():
        cross.wait_send()

    def sent(i, _):
        @pl.when(_first_order(chip, i) != chip)
        def _():
            for t in range(3):
                remote(i, t).wait_send()
        return 0

    lax.fori_loop(0, CHIPS - 1, sent, 0)
    start(CHIPS - 1, 2)

    def arrived(owner, _):
        for t in range(3):
            pltpu.make_async_copy((q_s, k_s, v_s)[t].at[0], place(t, owner), recv_sem.at[owner, t]).wait()
        return 0

    lax.fori_loop(0, CHIPS, arrived, 0)


def _finish(q_ref, k_ref, v_ref, x_ref, wo_ref, y_ref, q_s, k_s, v_s, x_s, o_s, o_r, acc_s, sum_r, w_s, top_s, mix_s, y_s,
            in_sem, w_sem, send_sem, recv_sem, sum_send, sum_recv, out_sem):
    me = lax.axis_index("sp")
    chip, core = lax.div(me, 2), lax.rem(me, 2)
    nh, total, _ = q_ref.shape
    own, d = x_ref.shape
    bq = 2 * own
    wide = nh * HEAD
    cols = d // TILES
    e = HEAD**-0.5 * LOG2E

    end = _at_end(chip)
    order = ((0, 0, 0), (0, 0, 1), (0, 1, 1), (0, 1, 0), (1, 1 - end, 1), (1, 1 - end, 0), (1, end, 1), (1, end, 0))

    def fetch(n, ct):
        first = (core * CHIPS + _partner(chip, *order[n])) * wide
        slot = _rem(ct if n < CHIPS - 2 else 2 * ct + n - (CHIPS - 2), SLOTS)
        return pltpu.make_async_copy(wo_ref.at[pl.ds(pl.multiple_of(first, HEAD), wide), pl.ds(pl.multiple_of(ct * cols, 128), cols)],
                                     w_s.at[slot], w_sem.at[slot])

    ins = [pltpu.make_async_copy(q_ref, q_s, in_sem.at[0]), pltpu.make_async_copy(k_ref, k_s, in_sem.at[1]),
           pltpu.make_async_copy(v_ref, v_s.at[:, :HEAD, :], in_sem.at[2]), pltpu.make_async_copy(x_ref, x_s, in_sem.at[3])]
    for copy in ins:
        copy.start()
    for ct in range(SLOTS):
        fetch(0, ct).start()
    v_s[:, HEAD:, :] = jnp.ones((nh, 16, total), jnp.bfloat16)
    _meet(core, chip)
    for copy in ins[:3]:
        copy.wait()

    def remote(i):
        return pltpu.make_async_remote_copy(src_ref=o_s.at[i], dst_ref=o_r.at[chip], send_sem=send_sem.at[i], recv_sem=recv_sem.at[chip],
                                            device_id={"sp": 2 * _second_order(chip, i) + core}, device_id_type=MESH)

    def strip(i, _):
        j = _second_order(chip, i)
        queries = pl.ds(pl.multiple_of(j * bq, bq), bq)

        def block(first, bk, masked):
            keys = pl.ds(pl.multiple_of(first, 256), bk)
            scores = [_dot(k_s[h, keys, :], q_s[h, queries, :], 1, 1) for h in range(nh)]
            if masked:
                ok = lax.broadcasted_iota(jnp.int32, (bk, bq), 0) - (bk - bq) <= lax.broadcasted_iota(jnp.int32, (bk, bq), 1)
            weights, keeps = [], []
            for h, s in enumerate(scores):
                if masked:
                    s = jnp.where(ok, s, HIDDEN)
                old = top_s[h : h + 1, :]
                top = jnp.maximum(old, s.max(axis=0, keepdims=True))
                top_s[h : h + 1, :] = top
                weights.append(jnp.exp2((s - top) * e).astype(jnp.bfloat16))
                keeps.append(jnp.exp2((old - top) * e))
            for h, (p, keep) in enumerate(zip(weights, keeps)):
                mix_s[h] = mix_s[h] * keep + _dot(v_s[h, :, keys], p)

        top_s[...] = jnp.full_like(top_s, NEG)
        mix_s[...] = jnp.zeros_like(mix_s)

        @pl.when(lax.rem(j, 2) == 1)
        def _():
            block((j - 1) * bq, 2 * bq, True)

        @pl.when(lax.rem(j, 2) == 0)
        def _():
            block(j * bq, bq, True)

        @pl.when(i > 0)
        def _():
            remote(i - 1).start()

        lax.fori_loop(0, lax.div(j, 2), lambda n, _: (block(n * 2 * bq, 2 * bq, False), 0)[1], 0)

        def store(ref, at):
            for h in range(nh):
                out = (mix_s[h, :HEAD, :] * (1 / mix_s[h, HEAD : HEAD + 1, :])).T
                ref[at, :, h * HEAD : (h + 1) * HEAD] = out.astype(jnp.bfloat16)

        @pl.when(i < CHIPS - 1)
        def _():
            store(o_s, i)

        @pl.when(i == CHIPS - 1)
        def _():
            store(o_r, chip)

        return 0

    lax.fori_loop(0, CHIPS, strip, 0)

    theirs, mine = (pl.ds(pl.multiple_of(c * own, own), own) for c in (1 - core, core))

    def columns(ct):
        return pl.ds(pl.multiple_of(ct * cols, 128), cols)

    def swap(ct):
        return pltpu.make_async_remote_copy(src_ref=acc_s.at[theirs, columns(ct)], dst_ref=sum_r.at[:, columns(ct)], send_sem=sum_send.at[ct],
                                            recv_sem=sum_recv.at[ct], device_id={"sp": 2 * chip + 1 - core}, device_id_type=MESH)

    def taken(n):
        source = _partner(chip, *order[n])
        if n:
            pltpu.make_async_copy(o_s.at[0], o_r.at[source], recv_sem.at[source]).wait()
        return source

    for n in range(CHIPS - 2):
        source = taken(n)

        def tile(ct, _):
            fetch(n, ct).wait()
            part = _dot(o_r[source], w_s[lax.rem(ct, SLOTS)])
            if n:
                part += acc_s[:, columns(ct)]
            acc_s[:, columns(ct)] = part

            @pl.when(ct < TILES - SLOTS)
            def _():
                fetch(n, ct + SLOTS).start()

            @pl.when(ct >= TILES - SLOTS)
            def _():
                if n < CHIPS - 3:
                    fetch(n + 1, ct - (TILES - SLOTS)).start()
                else:
                    for g in range(2):
                        @pl.when(lax.rem(ct, 2) == g)
                        def _():
                            fetch(CHIPS - 2 + g, lax.div(ct - (TILES - SLOTS), 2)).start()
            return 0

        lax.fori_loop(0, TILES, tile, 0)

    def result(ct):
        return pltpu.make_async_copy(y_s.at[:, columns(ct)], y_ref.at[:, columns(ct)], out_sem.at[ct])

    def add(ct):
        swap(ct).wait()
        y_s[:, columns(ct)] = (x_s[:, columns(ct)].astype(jnp.float32) + (acc_s[mine, columns(ct)] + sum_r[:, columns(ct)])).astype(jnp.bfloat16)

    ins[3].wait()
    sources = [taken(n) for n in (CHIPS - 2, CHIPS - 1)]

    def last_tile(ct, _):
        part = acc_s[:, columns(ct)]
        for g in range(2):
            fetch(CHIPS - 2 + g, ct).wait()
            part += _dot(o_r[sources[g]], w_s[lax.rem(2 * ct + g, SLOTS)])
        acc_s[:, columns(ct)] = part
        for g in range(2):
            @pl.when(ct < TILES - SLOTS // 2)
            def _():
                fetch(CHIPS - 2 + g, ct + SLOTS // 2).start()

        @pl.when(ct > 0)
        def _():
            swap(ct - 1).start()

        @pl.when(ct >= LAG)
        def _():
            add(ct - LAG)

        @pl.when(ct > LAG)
        def _():
            result(ct - LAG - 1).start()
        return 0

    lax.fori_loop(0, TILES, last_tile, 0)
    swap(TILES - 1).start()

    def rest(ct, _):
        add(ct)
        result(ct - 1).start()
        return 0

    lax.fori_loop(TILES - LAG, TILES, rest, 0)
    for i in range(CHIPS - 1):
        remote(i).wait_send()
    result(TILES - 1).start()
    for ct in range(TILES):
        result(ct).wait()


def solution(mesh):
    def step(x, gain, wq, wk, wv, wo):
        own, d = x.shape
        nh = wq.shape[1] // (2 * CHIPS * HEAD)
        total = 2 * CHIPS * own
        bf, f32 = jnp.bfloat16, jnp.float32
        hbm = pl.BlockSpec(memory_space=pl.ANY)
        vmem = pl.BlockSpec(memory_space=pltpu.VMEM)
        dma = pltpu.SemaphoreType.DMA

        chip = lax.div(lax.axis_index("sp"), 2)
        place = jnp.concatenate([c * 2 * own + jnp.arange(2 * own) for c in (chip, _across(chip))])
        half = HEAD // 2
        angle = place.astype(f32)[:, None] * THETA ** (-jnp.arange(half, dtype=f32) / half)
        cos, sin = jnp.cos(angle), jnp.sin(angle)

        heads = jax.ShapeDtypeStruct((nh, total, HEAD), bf)
        q, k, v = pl.pallas_call(
            _project,
            out_shape=[heads, heads, jax.ShapeDtypeStruct((nh, HEAD, total), bf)],
            in_specs=[hbm, vmem, vmem, vmem, hbm, hbm, hbm],
            out_specs=[hbm, hbm, hbm],
            scratch_shapes=[
                pltpu.VMEM((4 * own, d), bf),
                pltpu.VMEM((KCHUNKS, d // KCHUNKS, nh * HEAD), bf),
                pltpu.VMEM((2 * own, nh * HEAD), f32),
                pltpu.VMEM((CHIPS, nh, 2 * own, HEAD), bf),
                pltpu.VMEM((CHIPS, nh, 2 * own, HEAD), bf),
                pltpu.VMEM((CHIPS, nh, HEAD, 2 * own), bf),
                pltpu.VMEM((1, d), f32),
                pltpu.VMEM((4 * own, HEAD), f32),
                pltpu.VMEM((4 * own, HEAD), f32),
                dma, dma((3,)), dma((3,)), dma((KCHUNKS,)), dma((CHIPS, 3)), dma((CHIPS, 3)),
            ],
            compiler_params=pltpu.CompilerParams(collective_id=0, has_side_effects=True, vmem_limit_bytes=VMEM),
            name="project",
        )(x, gain.reshape(-1, 128), cos, sin, wq, wk, wv)

        return pl.pallas_call(
            _finish,
            out_shape=jax.ShapeDtypeStruct((own, wo.shape[1]), bf),
            in_specs=[hbm] * 5,
            out_specs=hbm,
            scratch_shapes=[
                pltpu.VMEM((nh, total, HEAD), bf),
                pltpu.VMEM((nh, total, HEAD), bf),
                pltpu.VMEM((nh, HEAD + 16, total), bf),
                pltpu.VMEM((own, d), bf),
                pltpu.VMEM((CHIPS, 2 * own, nh * HEAD), bf),
                pltpu.VMEM((CHIPS, 2 * own, nh * HEAD), bf),
                pltpu.VMEM((2 * own, d), f32),
                pltpu.VMEM((own, d), f32),
                pltpu.VMEM((SLOTS, nh * HEAD, d // TILES), bf),
                pltpu.VMEM((-(-nh // 8) * 8, 2 * own), f32),
                pltpu.VMEM((nh, HEAD + 16, 2 * own), f32),
                pltpu.VMEM((own, d), bf),
                dma((4,)), dma((SLOTS,)), dma((CHIPS,)), dma((CHIPS,)), dma((TILES,)), dma((TILES,)), dma((TILES,)),
            ],
            compiler_params=pltpu.CompilerParams(collective_id=1, has_side_effects=True, vmem_limit_bytes=VMEM),
            name="finish",
        )(q, k, v, x, wo)

    tokens, whole = P(("dp", "sp"), None), P(None, None)
    return jax.shard_map(
        step,
        mesh=mesh,
        in_specs=(tokens, P(None), whole, whole, whole, whole),
        out_specs=tokens,
        check_vma=False,
    )
```

```python
import functools

import jax
import jax.numpy as jnp
from jax import lax
from jax.experimental import pallas as pl
from jax.experimental.pallas import tpu as pltpu
from jax.sharding import PartitionSpec as P

HEAD = 128
THETA = 10000
CHIPS = 8
NEG = -1e30
HIDDEN = 2 * NEG
LOG2E = 1.4426950408889634
VMEM = 63 * 2**20
MESH = pl.DeviceIdType.MESH
KCHUNKS = 4
SLOTS = 6
TILES = 12
LAG = 4


def _dot(a, b, ca=1, cb=0):
    return lax.dot_general(a, b, (((ca,), (cb,)), ((), ())), preferred_element_type=jnp.float32)


def _partner(chip, far, b0, a):
    z, y = lax.rem(chip, 4), lax.div(chip, 4)
    z1, z0 = lax.div(z, 2), lax.rem(z, 2)
    z1 = z1 + far - 2 * z1 * far
    z0 = z0 + b0 - 2 * z0 * b0
    y = y + a - 2 * y * a
    return 4 * y + 2 * z1 + z0


def _div(i, n):
    return i // n if isinstance(i, int) else lax.div(i, n)


def _rem(i, n):
    return i % n if isinstance(i, int) else lax.rem(i, n)


def _at_end(chip):
    return 1 - lax.rem(lax.div(lax.rem(chip, 4) + 1, 2), 2)


def _across(chip):
    return _partner(chip, 1, 1, 0)


def _first_order(chip, i):
    end = _at_end(chip)
    far = end * _rem(_div(i + 2, 4), 2)
    b0 = end * (1 - _div(i, 4)) + (1 - end) * (1 - _div(_rem(i, 4), 2))
    return _partner(chip, far, b0, 1 - _rem(i, 2))


def _second_order(chip, i):
    end, y = _at_end(chip), _div(chip, 4)
    from2, from3, from4, from5, from7 = (_div(i + 8 - n, 8) for n in (2, 3, 4, 5, 7))
    p = _rem(i + end * from3 + (1 - end) * from5, 2)
    far = end * (from3 - from7) + (1 - end) * (1 - from2 + from5 - from7)
    beside = end * (from2 - from3) + (1 - end) * (from4 - from5)
    b0 = end * (1 - from5) * (1 - beside) + (1 - end) * (1 - from4)
    return _partner(chip, far, b0, beside + (1 - beside) * (1 - from7) * (y + p - 2 * y * p))


def _meet(core, chip):
    barrier = pltpu.get_barrier_semaphore()
    for code in range(1, CHIPS):
        other = _partner(chip, code // 4, code % 2, code // 2 % 2)
        pl.semaphore_signal(barrier, inc=1, device_id={"sp": 2 * other + core}, device_id_type=MESH)
    pl.semaphore_signal(barrier, inc=1, device_id={"sp": 2 * chip + 1 - core}, device_id_type=MESH)
    pl.semaphore_wait(barrier, CHIPS)


def _project(x_ref, gain_ref, cos_ref, sin_ref, wq_ref, wk_ref, wv_ref, q_ref, k_ref, v_ref,
             a_s, w_s, acc_s, q_s, k_s, v_s, gain_s, cos_s, sin_s, x_sem, x_send, x_recv, w_sem, send_sem, recv_sem):
    me = lax.axis_index("sp")
    chip, core = lax.div(me, 2), lax.rem(me, 2)
    middle = _at_end(chip) == 0
    own, d = x_ref.shape
    nh = q_ref.shape[0]
    wide = nh * HEAD
    deep = d // KCHUNKS
    weights = (wq_ref, wk_ref, wv_ref)

    def fetch(i, t, c):
        first = (core * CHIPS + _first_order(chip, i)) * wide
        return pltpu.make_async_copy(weights[t].at[pl.ds(c * deep, deep), pl.ds(pl.multiple_of(first, HEAD), wide)], w_s.at[c], w_sem.at[c])

    def second(i):
        return (1 - _at_end(chip)) * _div(i, 4)

    def place(t, owner):
        tokens = pl.ds(pl.multiple_of(owner * 2 * own, 2 * own), 2 * own)
        return (q_ref, k_ref)[t].at[:, tokens, :] if t < 2 else v_ref.at[:, :, tokens]

    def owner_of(i):
        return chip + second(i) * (_across(chip) - chip)

    def remote(i, t):
        owner = owner_of(i)
        return pltpu.make_async_remote_copy(src_ref=(q_s, k_s, v_s)[t].at[i], dst_ref=place(t, owner), send_sem=send_sem.at[i, t],
                                            recv_sem=recv_sem.at[owner, t], device_id={"sp": 2 * _first_order(chip, i) + core},
                                            device_id_type=MESH)

    def local(i, t):
        owner = owner_of(i)
        return pltpu.make_async_copy((q_s, k_s, v_s)[t].at[i], place(t, owner), recv_sem.at[owner, t])

    def start(i, t):
        here = _first_order(chip, i) == chip

        @pl.when(here)
        def _():
            local(i, t).start()

        @pl.when(jnp.logical_not(here))
        def _():
            remote(i, t).start()

    def block(n):
        return a_s.at[pl.ds(pl.multiple_of(n * own, own), own)]

    def push(n, src, dst, to):
        return pltpu.make_async_remote_copy(src_ref=src, dst_ref=dst, send_sem=x_send.at[n], recv_sem=x_recv.at[n],
                                            device_id={"sp": to}, device_id_type=MESH)

    swap = push(0, x_ref, block(core), 2 * chip + 1 - core)
    cross = push(1, x_ref, block(2 + core), 2 * _across(chip) + core)
    pass_on = push(2, block(2 + core), block(2 + core), 2 * chip + 1 - core)

    mine = pltpu.make_async_copy(x_ref, block(core), x_sem)
    mine.start()
    for c in range(KCHUNKS):
        fetch(0, 0, c).start()
    _meet(core, chip)
    swap.start()

    @pl.when(middle)
    def _():
        cross.start()

    gain_s[...] = jnp.concatenate([gain_ref[n : n + 1, :] for n in range(d // 128)], 1).astype(jnp.float32)
    cos_s[...] = jnp.concatenate([cos_ref[...], cos_ref[...]], 1)
    sin_s[...] = jnp.concatenate([-sin_ref[...], sin_ref[...]], 1)

    def norm(n):
        def some(r, _):
            at = pl.ds(pl.multiple_of(n * own + r * 16, 16), 16)
            x = a_s[at, :].astype(jnp.float32)
            scale = lax.rsqrt(jnp.mean(x * x, -1, keepdims=True) + 1e-6)
            a_s[at, :] = (a_s[at, :].astype(jnp.float32) * scale * gain_s[...]).astype(jnp.bfloat16)
            return 0

        lax.fori_loop(0, own // 16, some, 0)

    mine.wait()
    norm(core)
    swap.wait_recv()
    norm(1 - core)

    def chip_step(i, _):
        @pl.when(middle & (i == 4))
        def _():
            pass_on.wait_send()
            norm(2 + core)
            pass_on.wait_recv()
            norm(3 - core)

        rows = pl.ds(pl.multiple_of(second(i) * 2 * own, 2 * own), 2 * own)
        for t in range(3):
            acc_s[...] = jnp.zeros_like(acc_s)

            def piece(c, _):
                fetch(i, t, c).wait()
                acc_s[...] += _dot(a_s[rows, pl.ds(pl.multiple_of(c * deep, 128), deep)], w_s[c])
                if t < 2:
                    fetch(i, t + 1, c).start()
                else:
                    @pl.when(i < CHIPS - 1)
                    def _():
                        fetch(i + 1, 0, c).start()
                return 0

            lax.fori_loop(0, KCHUNKS, piece, 0)
            if t:
                start(i, t - 1)
            else:
                @pl.when(i > 0)
                def _():
                    start(i - 1, 2)
            for h in range(nh):
                part = acc_s[:, h * HEAD : (h + 1) * HEAD].astype(jnp.bfloat16)
                if t < 2:
                    part = part.astype(jnp.float32)
                    part = (part * cos_s[rows, :] + pltpu.roll(part, HEAD // 2, 1) * sin_s[rows, :]).astype(jnp.bfloat16)
                    (q_s, k_s)[t][i, h] = part
                else:
                    v_s[i, h] = part.T
            if t == 1:
                @pl.when(middle & (i == 3))
                def _():
                    cross.wait_recv()
                    pass_on.start()
        return 0

    lax.fori_loop(0, CHIPS, chip_step, 0)
    swap.wait_send()

    @pl.when(middle)
    def _():
        cross.wait_send()

    def sent(i, _):
        @pl.when(_first_order(chip, i) != chip)
        def _():
            for t in range(3):
                remote(i, t).wait_send()
        return 0

    lax.fori_loop(0, CHIPS - 1, sent, 0)
    start(CHIPS - 1, 2)

    def arrived(owner, _):
        for t in range(3):
            pltpu.make_async_copy((q_s, k_s, v_s)[t].at[0], place(t, owner), recv_sem.at[owner, t]).wait()
        return 0

    lax.fori_loop(0, CHIPS, arrived, 0)


def _finish(q_ref, k_ref, v_ref, x_ref, wo_ref, y_ref, q_s, k_s, v_s, x_s, o_s, o_r, acc_s, sum_r, w_s, top_s, mix_s, y_s,
            in_sem, w_sem, send_sem, recv_sem, sum_send, sum_recv, out_sem):
    me = lax.axis_index("sp")
    chip, core = lax.div(me, 2), lax.rem(me, 2)
    nh, total, _ = q_ref.shape
    own, d = x_ref.shape
    bq = 2 * own
    wide = nh * HEAD
    cols = d // TILES
    e = HEAD**-0.5 * LOG2E

    end = _at_end(chip)
    order = ((0, 0, 0), (0, 1 - end, 1), (0, 1, end), (0, end, 1 - end), (1, 1, 1), (1, 1, 0), (1, 0, 1), (1, 0, 0))

    def fetch(n, ct):
        first = (core * CHIPS + _partner(chip, *order[n])) * wide
        slot = _rem(ct if n < CHIPS - 2 else 2 * ct + n - (CHIPS - 2), SLOTS)
        return pltpu.make_async_copy(wo_ref.at[pl.ds(pl.multiple_of(first, HEAD), wide), pl.ds(pl.multiple_of(ct * cols, 128), cols)],
                                     w_s.at[slot], w_sem.at[slot])

    ins = [pltpu.make_async_copy(q_ref, q_s, in_sem.at[0]), pltpu.make_async_copy(k_ref, k_s, in_sem.at[1]),
           pltpu.make_async_copy(v_ref, v_s.at[:, :HEAD, :], in_sem.at[2]), pltpu.make_async_copy(x_ref, x_s, in_sem.at[3])]
    for copy in ins:
        copy.start()
    for ct in range(SLOTS):
        fetch(0, ct).start()
    v_s[:, HEAD:, :] = jnp.ones((nh, 16, total), jnp.bfloat16)
    _meet(core, chip)
    for copy in ins[:3]:
        copy.wait()

    def remote(i):
        return pltpu.make_async_remote_copy(src_ref=o_s.at[i], dst_ref=o_r.at[chip], send_sem=send_sem.at[i], recv_sem=recv_sem.at[chip],
                                            device_id={"sp": 2 * _second_order(chip, i) + core}, device_id_type=MESH)

    def strip(i, _):
        j = _second_order(chip, i)
        queries = pl.ds(pl.multiple_of(j * bq, bq), bq)

        def block(first, bk, masked):
            keys = pl.ds(pl.multiple_of(first, 256), bk)
            scores = [_dot(k_s[h, keys, :], q_s[h, queries, :], 1, 1) for h in range(nh)]
            if masked:
                ok = lax.broadcasted_iota(jnp.int32, (bk, bq), 0) - (bk - bq) <= lax.broadcasted_iota(jnp.int32, (bk, bq), 1)
            weights, keeps = [], []
            for h, s in enumerate(scores):
                if masked:
                    s = jnp.where(ok, s, HIDDEN)
                old = top_s[h : h + 1, :]
                top = jnp.maximum(old, s.max(axis=0, keepdims=True))
                top_s[h : h + 1, :] = top
                weights.append(jnp.exp2((s - top) * e).astype(jnp.bfloat16))
                keeps.append(jnp.exp2((old - top) * e))
            for h, (p, keep) in enumerate(zip(weights, keeps)):
                mix_s[h] = mix_s[h] * keep + _dot(v_s[h, :, keys], p)

        top_s[...] = jnp.full_like(top_s, NEG)
        mix_s[...] = jnp.zeros_like(mix_s)

        @pl.when(lax.rem(j, 2) == 1)
        def _():
            block((j - 1) * bq, 2 * bq, True)

        @pl.when(lax.rem(j, 2) == 0)
        def _():
            block(j * bq, bq, True)

        @pl.when(i > 0)
        def _():
            remote(i - 1).start()

        lax.fori_loop(0, lax.div(j, 2), lambda n, _: (block(n * 2 * bq, 2 * bq, False), 0)[1], 0)

        def store(ref, at):
            for h in range(nh):
                out = (mix_s[h, :HEAD, :] * (1 / mix_s[h, HEAD : HEAD + 1, :])).T
                ref[at, :, h * HEAD : (h + 1) * HEAD] = out.astype(jnp.bfloat16)

        @pl.when(i < CHIPS - 1)
        def _():
            store(o_s, i)

        @pl.when(i == CHIPS - 1)
        def _():
            store(o_r, chip)

        return 0

    lax.fori_loop(0, CHIPS, strip, 0)

    theirs, mine = (pl.ds(pl.multiple_of(c * own, own), own) for c in (1 - core, core))

    def columns(ct):
        return pl.ds(pl.multiple_of(ct * cols, 128), cols)

    def swap(ct):
        return pltpu.make_async_remote_copy(src_ref=acc_s.at[theirs, columns(ct)], dst_ref=sum_r.at[:, columns(ct)], send_sem=sum_send.at[ct],
                                            recv_sem=sum_recv.at[ct], device_id={"sp": 2 * chip + 1 - core}, device_id_type=MESH)

    def taken(n):
        source = _partner(chip, *order[n])
        if n:
            pltpu.make_async_copy(o_s.at[0], o_r.at[source], recv_sem.at[source]).wait()
        return source

    for n in range(CHIPS - 2):
        source = taken(n)

        def tile(ct, _):
            fetch(n, ct).wait()
            part = _dot(o_r[source], w_s[lax.rem(ct, SLOTS)])
            if n:
                part += acc_s[:, columns(ct)]
            acc_s[:, columns(ct)] = part

            @pl.when(ct < TILES - SLOTS)
            def _():
                fetch(n, ct + SLOTS).start()

            @pl.when(ct >= TILES - SLOTS)
            def _():
                if n < CHIPS - 3:
                    fetch(n + 1, ct - (TILES - SLOTS)).start()
                else:
                    for g in range(2):
                        @pl.when(lax.rem(ct, 2) == g)
                        def _():
                            fetch(CHIPS - 2 + g, lax.div(ct - (TILES - SLOTS), 2)).start()
            return 0

        lax.fori_loop(0, TILES, tile, 0)

    def result(ct):
        return pltpu.make_async_copy(y_s.at[:, columns(ct)], y_ref.at[:, columns(ct)], out_sem.at[ct])

    def add(ct):
        swap(ct).wait()
        y_s[:, columns(ct)] = (x_s[:, columns(ct)].astype(jnp.float32) + (acc_s[mine, columns(ct)] + sum_r[:, columns(ct)])).astype(jnp.bfloat16)

    ins[3].wait()
    sources = [taken(n) for n in (CHIPS - 2, CHIPS - 1)]

    def last_tile(ct, _):
        part = acc_s[:, columns(ct)]
        for g in range(2):
            fetch(CHIPS - 2 + g, ct).wait()
            part += _dot(o_r[sources[g]], w_s[lax.rem(2 * ct + g, SLOTS)])
        acc_s[:, columns(ct)] = part
        for g in range(2):
            @pl.when(ct < TILES - SLOTS // 2)
            def _():
                fetch(CHIPS - 2 + g, ct + SLOTS // 2).start()

        @pl.when(ct > 0)
        def _():
            swap(ct - 1).start()

        @pl.when(ct >= LAG)
        def _():
            add(ct - LAG)

        @pl.when(ct > LAG)
        def _():
            result(ct - LAG - 1).start()
        return 0

    lax.fori_loop(0, TILES, last_tile, 0)
    swap(TILES - 1).start()

    def rest(ct, _):
        add(ct)
        result(ct - 1).start()
        return 0

    lax.fori_loop(TILES - LAG, TILES, rest, 0)
    for i in range(CHIPS - 1):
        remote(i).wait_send()
    result(TILES - 1).start()
    for ct in range(TILES):
        result(ct).wait()


def solution(mesh):
    def step(x, gain, wq, wk, wv, wo):
        own, d = x.shape
        nh = wq.shape[1] // (2 * CHIPS * HEAD)
        total = 2 * CHIPS * own
        bf, f32 = jnp.bfloat16, jnp.float32
        hbm = pl.BlockSpec(memory_space=pl.ANY)
        vmem = pl.BlockSpec(memory_space=pltpu.VMEM)
        dma = pltpu.SemaphoreType.DMA

        chip = lax.div(lax.axis_index("sp"), 2)
        place = jnp.concatenate([c * 2 * own + jnp.arange(2 * own) for c in (chip, _across(chip))])
        half = HEAD // 2
        angle = place.astype(f32)[:, None] * THETA ** (-jnp.arange(half, dtype=f32) / half)
        cos, sin = jnp.cos(angle), jnp.sin(angle)

        heads = jax.ShapeDtypeStruct((nh, total, HEAD), bf)
        q, k, v = pl.pallas_call(
            _project,
            out_shape=[heads, heads, jax.ShapeDtypeStruct((nh, HEAD, total), bf)],
            in_specs=[hbm, vmem, vmem, vmem, hbm, hbm, hbm],
            out_specs=[hbm, hbm, hbm],
            scratch_shapes=[
                pltpu.VMEM((4 * own, d), bf),
                pltpu.VMEM((KCHUNKS, d // KCHUNKS, nh * HEAD), bf),
                pltpu.VMEM((2 * own, nh * HEAD), f32),
                pltpu.VMEM((CHIPS, nh, 2 * own, HEAD), bf),
                pltpu.VMEM((CHIPS, nh, 2 * own, HEAD), bf),
                pltpu.VMEM((CHIPS, nh, HEAD, 2 * own), bf),
                pltpu.VMEM((1, d), f32),
                pltpu.VMEM((4 * own, HEAD), f32),
                pltpu.VMEM((4 * own, HEAD), f32),
                dma, dma((3,)), dma((3,)), dma((KCHUNKS,)), dma((CHIPS, 3)), dma((CHIPS, 3)),
            ],
            compiler_params=pltpu.CompilerParams(collective_id=0, has_side_effects=True, vmem_limit_bytes=VMEM),
            name="project",
        )(x, gain.reshape(-1, 128), cos, sin, wq, wk, wv)

        return pl.pallas_call(
            _finish,
            out_shape=jax.ShapeDtypeStruct((own, wo.shape[1]), bf),
            in_specs=[hbm] * 5,
            out_specs=hbm,
            scratch_shapes=[
                pltpu.VMEM((nh, total, HEAD), bf),
                pltpu.VMEM((nh, total, HEAD), bf),
                pltpu.VMEM((nh, HEAD + 16, total), bf),
                pltpu.VMEM((own, d), bf),
                pltpu.VMEM((CHIPS, 2 * own, nh * HEAD), bf),
                pltpu.VMEM((CHIPS, 2 * own, nh * HEAD), bf),
                pltpu.VMEM((2 * own, d), f32),
                pltpu.VMEM((own, d), f32),
                pltpu.VMEM((SLOTS, nh * HEAD, d // TILES), bf),
                pltpu.VMEM((-(-nh // 8) * 8, 2 * own), f32),
                pltpu.VMEM((nh, HEAD + 16, 2 * own), f32),
                pltpu.VMEM((own, d), bf),
                dma((4,)), dma((SLOTS,)), dma((CHIPS,)), dma((CHIPS,)), dma((TILES,)), dma((TILES,)), dma((TILES,)),
            ],
            compiler_params=pltpu.CompilerParams(collective_id=1, has_side_effects=True, vmem_limit_bytes=VMEM),
            name="finish",
        )(q, k, v, x, wo)

    tokens, whole = P(("dp", "sp"), None), P(None, None)
    return jax.shard_map(
        step,
        mesh=mesh,
        in_specs=(tokens, P(None), whole, whole, whole, whole),
        out_specs=tokens,
        check_vma=False,
    )
```
